256 devices in a mesh: section: 8 (over x, core), paths: 32 (over y, z).
Axes of the slice: x: 4, y: 4, z: 8, core: 2. Of those that a mesh axis runs over, the one named last changes fastest.
Arguments:
- normal_draws: float32 [16, 60, 32768], P('section', None, 'paths'), may hold values from -6 to 6
- cholesky: float32 [16, 32, 60, 60], P('section', 'paths'), as said below
- log_spot: float32 [60], replicated, may hold values from -0.2 to 0.2
- owner: int32 [16], replicated, may hold values from 0 to 31
- trade_factor: int32 [4096], replicated, may hold values from 0 to 59
- trade_set: int32 [4096], replicated, may hold values from 0 to 511
- notional: float32 [4096], replicated, may hold values from -5 to 5
- strike: float32 [4096], replicated, may hold values from 0.8 to 1.25
Outputs:
- exposure: float32 [16, 512], P('section')
The draws below stay inside these ranges and needn't reach their ends.
Inputs may be any that keep to these rules, and one draw needn't show every extreme that they name: `cholesky`: each block is lower triangular with a positive diagonal.
All inputs are finite; a program needn't handle non-finite values.
Results may differ from the reference program's by a relative error of at most 0.0001.
Values sent between devices are 32-bit elements; how exact they have to be, the bound alone decides.
A program may use at most 64 MiB of HBM per device.

```python
import jax
import jax.numpy as jnp
from jax import lax

F = 60
TRADES = 4096
SETS = 512
DATES = 16
OWNERS = 32
PATHS = 32768


def draw_cholesky(key, part):
    first, second = jax.random.split(jax.random.fold_in(key, 17))
    diagonal = jax.random.uniform(first, (DATES, OWNERS, F), jnp.float32, 0.5, 1.5)
    spread = jax.random.normal(second, (DATES, OWNERS, F, F), jnp.float32) * (0.5 / F ** 0.5)
    lower = jnp.tril(spread, -1) + diagonal[..., None] * jnp.eye(F, dtype=jnp.float32)
    return (0.1 * lower).astype(jnp.float32)


def with_ends(result, own_key, low, largest):
    extent = result.shape
    place = [jax.random.randint(jax.random.fold_in(own_key, axis), (), 0, extent[axis]) for axis in range(len(extent))]
    result = result.at[tuple(place)].set(low)
    longest = extent.index(max(extent))
    place[longest] = (place[longest] + 1) % extent[longest]
    return result.at[tuple(place)].set(largest)


def level_of(key, shape, cuts, smallest, high):
    gain, own = 1.0, jax.random.fold_in(key, 6)
    for dim, parts in cuts:
        heights = jnp.exp(jax.random.uniform(jax.random.fold_in(own, dim), (parts,), jnp.float32, smallest / len(cuts), high / len(cuts)))
        gain = gain * jnp.repeat(heights, shape[dim] // parts).reshape([-1 if axis == dim else 1 for axis in range(len(shape))])
    return gain


def bell_draw(own_key, extent, deviation, most, pieces=(), held_as=jnp.bfloat16):
    factor_of = level_of(own_key, extent, pieces, -0.22, 0.18) if pieces else 1.0
    drawn = jax.random.normal(own_key, extent, jnp.float32) * deviation * factor_of
    return jnp.minimum(jnp.maximum(drawn, -most), most).astype(held_as)


def setup_inputs(seed: int = 0) -> dict:
    key_list = jax.random.split(jax.random.key(seed), 9)
    return {
        "normal_draws": bell_draw(key_list[0], (DATES, F, PATHS), 1.0, 6.0, ((0, 8), (2, 32)), jnp.float32),
        "cholesky": draw_cholesky(jax.random.fold_in(key_list[8], 71), 0),
        "log_spot": jnp.clip(jax.random.uniform(key_list[2], (F,), jnp.float32, -0.2, 0.2), -0.2, 0.2),
        "owner": with_ends(jax.random.randint(key_list[3], (DATES,), 0, OWNERS), jax.random.fold_in(key_list[3], 1), 0, OWNERS - 1).astype(jnp.int32),
        "trade_factor": with_ends(jax.random.randint(key_list[4], (TRADES,), 0, F), jax.random.fold_in(key_list[4], 1), 0, F - 1).astype(jnp.int32),
        "trade_set": with_ends(jax.random.randint(key_list[5], (TRADES,), 0, SETS), jax.random.fold_in(key_list[5], 1), 0, SETS - 1).astype(jnp.int32),
        "notional": bell_draw(key_list[6], (TRADES,), 1.0, 5.0, (), jnp.float32),
        "strike": jnp.clip(jax.random.uniform(key_list[7], (TRADES,), jnp.float32, 0.8, 1.25), 0.8, 1.25),
    }


def reference(normal_draws, cholesky, log_spot, owner, trade_factor, trade_set, notional, strike):
    level = jnp.zeros((F, PATHS), jnp.float32) + log_spot[:, None]
    results = []
    for date in range(DATES):
        lower = cholesky[date, owner[date]]
        increment = jnp.dot(lower, normal_draws[date], precision=lax.Precision.HIGHEST, preferred_element_type=jnp.float32)
        level = level + increment
        price = jnp.exp(level)[trade_factor]
        payoff = notional[:, None] * jnp.maximum(price - strike[:, None], 0.0)
        net = jax.ops.segment_sum(payoff, trade_set, num_segments=SETS)
        results.append(jnp.sum(jnp.maximum(net, 0.0), axis=1) / PATHS)
    return jnp.stack(results, axis=0)
```

```python
import functools

import jax
import jax.numpy as jnp
from jax import lax
from jax.experimental import pallas as pl
from jax.experimental.pallas import tpu as pltpu
from jax.sharding import PartitionSpec as P

SETS = 512
TRADES = 4096
LANES = 128
ROWS = TRADES // LANES
HALF = TRADES // 2
MESH = pl.DeviceIdType.MESH
HIGHEST = lax.Precision.HIGHEST
F32 = jnp.float32
I32 = jnp.int32


def iota(shape, axis):
    return lax.broadcasted_iota(I32, shape, axis)


def remote(src, dst, send, recv, device):
    return pltpu.make_async_remote_copy(
        src_ref=src, dst_ref=dst, send_sem=send, recv_sem=recv, device_id=device, device_id_type=MESH
    )


def packed(first, second):
    row, col = iota((64, LANES), 0), iota((64, LANES), 1)
    across = jnp.transpose(second)[:64]
    square = jnp.where(col <= row, first[:64], across)
    diagonal = jnp.sum(jnp.where(col == row, second[:64], 0.0), axis=0, keepdims=True)
    square = jnp.where(row == 60, diagonal, square)
    return jnp.where(col[:32] < 64, square[:32], pltpu.roll(square[32:], 64, 1))


def unpacked(both):
    row, col = iota((64, LANES), 0), iota((64, LANES), 1)
    square = jnp.concatenate([both, pltpu.roll(both, 64, 1)], axis=0)
    square = jnp.where(col < 64, square, 0.0)
    first = jnp.where((col <= row) & (row < 60), square, 0.0)
    across = jnp.transpose(jnp.concatenate([square, jnp.zeros_like(square)], axis=0))[:64]
    second = jnp.where(col < row, across, 0.0)
    second = jnp.where(col == row, square[60:61], second)
    return first, jnp.where(row < 60, second, 0.0)


def partner(x, bit):
    if bit < 2:
        step = 1 << bit
        return [x[place ^ step] for place in range(4)]
    axis, step, extent = (0, 1 << (bit - 2), 8) if bit < 5 else (1, 1 << (bit - 5), LANES)
    upper = (iota((8, LANES), axis) & step) != 0
    return [
        jnp.where(upper, pltpu.roll(v, step, axis), pltpu.roll(v, extent - step, axis)) for v in x
    ]


def place_bit(bit, vreg):
    if bit < 2:
        return jnp.full((8, LANES), (vreg >> bit) & 1, I32)
    axis, shift = (0, bit - 2) if bit < 5 else (1, bit - 5)
    return (iota((8, LANES), axis) >> shift) & 1


def in_set_order(keys, carried):
    for level in range(1, 13):
        for bit in range(level - 1, -1, -1):
            other = partner(keys, bit)
            others = [partner(c, bit) for c in carried]
            new_keys, news = [], [[] for _ in carried]
            for v in range(4):
                upward = place_bit(level, v) if level < 12 else jnp.zeros((8, LANES), I32)
                wants_small = place_bit(bit, v) == upward
                swap = jnp.where(wants_small, keys[v] - other[v], other[v] - keys[v]) > 0
                new_keys.append(jnp.where(swap, other[v], keys[v]))
                for new, c, o in zip(news, carried, others):
                    new.append(jnp.where(swap, o[v], c[v]))
            keys, carried = new_keys, news
    return keys, carried


def kernel(
    sections, ys, zs, factors,
    draws, chol, spot, owner, tfactor, tset, notional, strike, out,
    chol_in, spot_in, owner_in, trades_in, trades_f_in, pack_a, pack_b,
    mine, over_y, y_sum, over_z, blocks, z_all, prices, order, order_in, ends, ends_in,
    strikes, notionals, keeps, nets, sums, over_x, x_sum, over_fy, fy_sum, over_fz,
    in_sems, order_sem, ends_sem, own_sem, y_send, y_recv, z_send, z_recv, x_send, x_recv,
    d_send, d_recv, fx_send, fx_recv, fy_send, fy_recv, fz_send, fz_recv,
):
    dates = 2 * sections
    section = lax.axis_index("section")
    place = lax.axis_index("paths")
    y, z = lax.div(place, zs), lax.rem(place, zs)
    y_peers = [(section, lax.rem(y + i, ys) * zs + z) for i in range(1, ys)]
    z_peers = [(section, y * zs + lax.rem(z + i, zs)) for i in range(1, zs)]
    x_peers = [(lax.rem(section + i, sections), place) for i in range(1, sections)]

    barrier = pltpu.get_barrier_semaphore()
    for peer in y_peers + z_peers + x_peers:
        pl.semaphore_signal(barrier, inc=1, device_id=peer, device_id_type=MESH)

    loads = [
        pltpu.make_async_copy(chol, chol_in, in_sems.at[0]),
        pltpu.make_async_copy(owner, owner_in, in_sems.at[1]),
        pltpu.make_async_copy(spot, spot_in, in_sems.at[2]),
        pltpu.make_async_copy(tfactor, trades_in.at[0], in_sems.at[3]),
        pltpu.make_async_copy(tset, trades_in.at[1], in_sems.at[4]),
        pltpu.make_async_copy(notional, trades_f_in.at[0], in_sems.at[5]),
        pltpu.make_async_copy(strike, trades_f_in.at[1], in_sems.at[6]),
    ]
    for load in loads:
        load.start()
    own = pltpu.make_async_copy(
        draws.at[:, :, pl.ds(pl.multiple_of(section * LANES, LANES), LANES)],
        z_all.at[section, :, pl.ds(0, factors), :],
        own_sem,
    )
    own.start()

    pack_a[...] = jnp.zeros_like(pack_a)
    pack_b[...] = jnp.zeros_like(pack_b)
    for e in range(sections):
        for d in range(2):
            z_all[e, d, factors:64, :] = jnp.zeros((64 - factors, LANES), F32)
    loads[0].wait()
    loads[1].wait()
    pack_a[0:factors, 0:factors] = jnp.where(owner_in[2 * section] == place, chol_in[0], 0.0)
    pack_b[0:factors, 0:factors] = jnp.where(owner_in[2 * section + 1] == place, chol_in[1], 0.0)
    mine[...] = packed(pack_a[...], pack_b[...])

    pl.semaphore_wait(barrier, len(y_peers) + len(z_peers) + len(x_peers))

    to_y = [
        remote(mine, over_y.at[i], y_send.at[i], y_recv.at[i], peer) for i, peer in enumerate(y_peers)
    ]
    for copy in to_y:
        copy.start()
    to_d = [
        remote(
            draws.at[:, :, pl.ds(pl.multiple_of(peer[0] * LANES, LANES), LANES)],
            z_all.at[section, :, pl.ds(0, factors), :],
            d_send.at[i], d_recv.at[i], peer,
        )
        for i, peer in enumerate(x_peers)
    ]
    for copy in to_d:
        copy.start()

    for load in loads[2:]:
        load.wait()
    keys = [
        trades_in[1, 8 * v:8 * v + 8, :] * 64 + trades_in[0, 8 * v:8 * v + 8, :] for v in range(4)
    ]
    carried = [[trades_f_in[a, 8 * v:8 * v + 8, :] for v in range(4)] for a in range(2)]
    keys, (notional_s, strike_s) = in_set_order(keys, carried)
    for v in range(4):
        order[8 * v:8 * v + 8, :] = keys[v] & 63
    to_order = pltpu.make_async_copy(order, order_in, order_sem)
    to_order.start()

    total = mine[...]
    for i, copy in enumerate(to_y):
        copy.wait_recv()
        total = total + over_y[i]
    y_sum[...] = total
    to_z = [
        remote(y_sum, over_z.at[i], z_send.at[i], z_recv.at[i], peer) for i, peer in enumerate(z_peers)
    ]
    for copy in to_z:
        copy.start()

    set_s = [k >> 6 for k in keys]
    sub, lane = iota((8, LANES), 0), iota((8, LANES), 1)
    down = pltpu.roll(set_s[3], 1, 0)
    before = [jnp.where(sub == 0, pltpu.roll(down, 1, 1), down), set_s[0], set_s[1], set_s[2]]
    keep_s = []
    for v in range(4):
        same = jnp.where(before[v] == set_s[v], 1.0, 0.0)
        if v == 0:
            same = jnp.where((sub == 0) & ((lane == 0) | (lane == LANES // 2)), 0.0, same)
        keep_s.append(same)
    for c in range(LANES):
        for v in range(4):
            at = pl.ds(c * 32 + 8 * v, 8)
            strikes[at, :] = jnp.broadcast_to(strike_s[v][:, c:c + 1], (8, LANES))
            notionals[at, :] = jnp.broadcast_to(notional_s[v][:, c:c + 1], (8, LANES))
            keeps[at, :] = jnp.broadcast_to(keep_s[v][:, c:c + 1], (8, LANES))

    counts = jnp.zeros((8, LANES), F32)
    low = iota((LANES, LANES), 0)
    for r in range(ROWS):
        sets = trades_in[1, r:r + 1, :]
        fine = jnp.where((sets & 127) == low, 1.0, 0.0)
        coarse = jnp.where((sets >> 7) == sub, 1.0, 0.0)
        counts = counts + lax.dot_general(
            coarse, fine, (((1,), (1,)), ((), ())), preferred_element_type=F32
        )
    upto = jnp.where(low <= iota((LANES, LANES), 1), 1.0, 0.0)
    through = jnp.dot(counts, upto, precision=HIGHEST, preferred_element_type=F32)
    offset = jnp.zeros((8, 1), F32)
    for h in range(SETS // LANES - 1):
        offset = offset + jnp.where(iota((8, 1), 0) > h, through[h:h + 1, LANES - 1:], 0.0)
    through = (through + offset).astype(I32)
    counts = counts.astype(I32)
    ends[0] = jnp.where(counts > 0, through - 1, TRADES)
    ends[1] = jnp.where((through - counts < HALF) & (through > HALF), HALF - 1, TRADES)
    to_ends = pltpu.make_async_copy(ends, ends_in, ends_sem)
    to_ends.start()

    spots = jnp.concatenate([spot_in[...], jnp.zeros((1, LANES - factors), F32)], axis=1)
    level = jnp.transpose(jnp.broadcast_to(spots, (LANES, LANES)))[:64]
    nets[TRADES] = jnp.zeros((dates, LANES), F32)

    total = y_sum[...]
    for i, copy in enumerate(to_z):
        copy.wait_recv()
        total = total + over_z[i]
    blocks[section] = total
    to_x = [
        remote(blocks.at[section], blocks.at[section], x_send.at[i], x_recv.at[i], peer)
        for i, peer in enumerate(x_peers)
    ]
    for copy in to_x:
        copy.start()
    own.wait()
    to_order.wait()
    to_ends.wait()
    for copy in to_d:
        copy.wait_recv()
    for copy in to_x:
        copy.wait_recv()

    for e in range(sections):
        for d, lower in enumerate(unpacked(blocks[e])):
            level = level + jnp.dot(
                lower[:, :64], z_all[e, d], precision=HIGHEST, preferred_element_type=F32
            )
            prices[:, 2 * e + d, :] = jnp.exp(level)

    def some_trades(c, accs):
        accs = list(accs)
        for j in range(32):
            row = (j & 3) * 8 + (j >> 2)
            for half in range(2):
                column = c + half * (LANES // 2)
                at = pl.ds(column * 32 + row, 1)
                price = prices[order_in[row, column]]
                payoff = notionals[at, :] * jnp.maximum(price - strikes[at, :], 0.0)
                accs[half] = accs[half] * keeps[at, :] + payoff
                nets[column * 32 + j] = accs[half]
        return tuple(accs)

    zero = jnp.zeros((dates, LANES), F32)
    lax.fori_loop(0, LANES // 2, some_trades, (zero, zero))

    lanes = iota((dates, LANES), 1)
    step = 32
    for b in range(SETS // LANES):
        def some_sets(q, sums_b):
            for i in range(step):
                at = q * step + i
                last, halfway = (jnp.clip(ends_in[a, b, at], 0, TRADES) for a in range(2))
                net = nets[last] + nets[halfway]
                sum_s = jnp.sum(jnp.maximum(net, 0.0), axis=1, keepdims=True)
                sums_b = jnp.where(lanes == at, sum_s, sums_b)
            return sums_b

        sums_b = lax.fori_loop(0, LANES // step, some_sets, jnp.zeros((dates, LANES), F32))
        for d in range(dates):
            sums[4 * d + b:4 * d + b + 1, :] = sums_b[d:d + 1]

    def rows_of(s):
        return sums.at[pl.ds(pl.multiple_of(s * 8, 8), 8), :]

    to_fx = [
        remote(rows_of(peer[0]), over_x.at[i], fx_send.at[i], fx_recv.at[i], peer)
        for i, peer in enumerate(x_peers)
    ]
    for copy in to_fx:
        copy.start()
    total = sums[pl.ds(pl.multiple_of(section * 8, 8), 8), :]
    for i, copy in enumerate(to_fx):
        copy.wait_recv()
        total = total + over_x[i]
    x_sum[...] = total
    to_fy = [
        remote(x_sum, over_fy.at[i], fy_send.at[i], fy_recv.at[i], peer)
        for i, peer in enumerate(y_peers)
    ]
    for copy in to_fy:
        copy.start()
    for i, copy in enumerate(to_fy):
        copy.wait_recv()
        total = total + over_fy[i]
    fy_sum[...] = total
    to_fz = [
        remote(fy_sum, over_fz.at[i], fz_send.at[i], fz_recv.at[i], peer)
        for i, peer in enumerate(z_peers)
    ]
    for copy in to_fz:
        copy.start()
    for i, copy in enumerate(to_fz):
        copy.wait_recv()
        total = total + over_fz[i]
    out[...] = total
    for copies in (to_y, to_z, to_x, to_d, to_fx, to_fy, to_fz):
        for copy in copies:
            copy.wait_send()


def shards(sections, ys, zs, normal_draws, cholesky, log_spot, owner, trade_factor, trade_set, notional, strike):
    factors = normal_draws.shape[1]
    dates = 2 * sections
    dma = pltpu.SemaphoreType.DMA
    vmem = pltpu.VMEM
    square = (ROWS, LANES)
    totals = pl.pallas_call(
        functools.partial(kernel, sections, ys, zs, factors),
        out_shape=jax.ShapeDtypeStruct((8, LANES), F32),
        in_specs=[pl.BlockSpec(memory_space=pl.ANY)] * 8,
        out_specs=pl.BlockSpec(memory_space=pltpu.VMEM),
        scratch_shapes=[
            vmem((2, factors, factors), F32),
            vmem((1, factors), F32),
            pltpu.SMEM((dates,), I32),
            vmem((2, *square), I32),
            vmem((2, *square), F32),
            vmem((LANES, LANES), F32),
            vmem((LANES, LANES), F32),
            vmem((32, LANES), F32),
            vmem((ys - 1, 32, LANES), F32),
            vmem((32, LANES), F32),
            vmem((zs - 1, 32, LANES), F32),
            vmem((sections, 32, LANES), F32),
            vmem((sections, 2, 64, LANES), F32),
            vmem((64, dates, LANES), F32),
            vmem(square, I32),
            pltpu.SMEM(square, I32),
            vmem((2, 8, LANES), I32),
            pltpu.SMEM((2, 8, LANES), I32),
            vmem((TRADES, LANES), F32),
            vmem((TRADES, LANES), F32),
            vmem((TRADES, LANES), F32),
            vmem((TRADES + 1, dates, LANES), F32),
            vmem((4 * dates, LANES), F32),
            vmem((sections - 1, 8, LANES), F32),
            vmem((8, LANES), F32),
            vmem((ys - 1, 8, LANES), F32),
            vmem((8, LANES), F32),
            vmem((zs - 1, 8, LANES), F32),
            dma((7,)), dma, dma, dma,
            dma((ys - 1,)), dma((ys - 1,)), dma((zs - 1,)), dma((zs - 1,)),
            dma((sections - 1,)), dma((sections - 1,)), dma((sections - 1,)), dma((sections - 1,)),
            dma((sections - 1,)), dma((sections - 1,)), dma((ys - 1,)), dma((ys - 1,)),
            dma((zs - 1,)), dma((zs - 1,)),
        ],
        compiler_params=pltpu.CompilerParams(
            collective_id=0, has_side_effects=True, vmem_limit_bytes=60 * 1024 * 1024
        ),
    )(
        normal_draws, cholesky[:, 0], log_spot.reshape(1, factors), owner,
        trade_factor.reshape(square), trade_set.reshape(square),
        notional.reshape(square), strike.reshape(square),
    )
    paths = normal_draws.shape[2] * ys * zs
    return totals.reshape(2, SETS) / paths


def solution(mesh):
    placed = (
        P("section", None, "paths"),
        P("section", "paths", None, None),
        P(), P(), P(), P(), P(), P(),
    )
    sections, paths = mesh.shape["section"], mesh.shape["paths"]
    zs = 8 if paths == 32 else 2
    return jax.shard_map(
        functools.partial(shards, sections, paths // zs, zs),
        mesh=mesh, in_specs=placed, out_specs=P("section", None), check_vma=False,
    )
```

```python
import functools

import jax
import jax.numpy as jnp
from jax import lax
from jax.experimental import pallas as pl
from jax.experimental.pallas import tpu as pltpu
from jax.sharding import PartitionSpec as P

SETS = 512
TRADES = 4096
LANES = 128
ROWS = TRADES // LANES
HALF = TRADES // 2
CHUNKS = 2
MESH = pl.DeviceIdType.MESH
HIGHEST = lax.Precision.HIGHEST
F32 = jnp.float32
I32 = jnp.int32


def iota(shape, axis):
    return lax.broadcasted_iota(I32, shape, axis)


def remote(src, dst, send, recv, device):
    return pltpu.make_async_remote_copy(
        src_ref=src, dst_ref=dst, send_sem=send, recv_sem=recv, device_id=device, device_id_type=MESH
    )


def packed(first, second):
    row, col = iota((64, LANES), 0), iota((64, LANES), 1)
    across = jnp.transpose(second)[:64]
    square = jnp.where(col <= row, first[:64], across)
    diagonal = jnp.sum(jnp.where(col == row, second[:64], 0.0), axis=0, keepdims=True)
    square = jnp.where(row == 60, diagonal, square)
    return jnp.where(col[:32] < 64, square[:32], pltpu.roll(square[32:], 64, 1))


def unpacked(both):
    row, col = iota((64, LANES), 0), iota((64, LANES), 1)
    square = jnp.concatenate([both, pltpu.roll(both, 64, 1)], axis=0)
    square = jnp.where(col < 64, square, 0.0)
    first = jnp.where((col <= row) & (row < 60), square, 0.0)
    across = jnp.transpose(jnp.concatenate([square, jnp.zeros_like(square)], axis=0))[:64]
    second = jnp.where(col < row, across, 0.0)
    second = jnp.where(col == row, square[60:61], second)
    return first, jnp.where(row < 60, second, 0.0)


def halves(x):
    high = x.astype(jnp.bfloat16).astype(F32)
    return high, x - high


def partner(x, bit):
    if bit < 2:
        step = 1 << bit
        return [x[place ^ step] for place in range(4)]
    axis, step, extent = (0, 1 << (bit - 2), 8) if bit < 5 else (1, 1 << (bit - 5), LANES)
    upper = (iota((8, LANES), axis) & step) != 0
    return [
        jnp.where(upper, pltpu.roll(v, step, axis), pltpu.roll(v, extent - step, axis)) for v in x
    ]


def place_bit(bit, vreg):
    if bit < 2:
        return jnp.full((8, LANES), (vreg >> bit) & 1, I32)
    axis, shift = (0, bit - 2) if bit < 5 else (1, bit - 5)
    return (iota((8, LANES), axis) >> shift) & 1


def in_set_order(keys, carried):
    for level in range(1, 13):
        for bit in range(level - 1, -1, -1):
            other = partner(keys, bit)
            others = [partner(c, bit) for c in carried]
            new_keys, news = [], [[] for _ in carried]
            for v in range(4):
                upward = place_bit(level, v) if level < 12 else jnp.zeros((8, LANES), I32)
                wants_small = place_bit(bit, v) == upward
                swap = jnp.where(wants_small, keys[v] - other[v], other[v] - keys[v]) > 0
                new_keys.append(jnp.where(swap, other[v], keys[v]))
                for new, c, o in zip(news, carried, others):
                    new.append(jnp.where(swap, o[v], c[v]))
            keys, carried = new_keys, news
    return keys, carried


def kernel(
    sections, ys, zs, factors, paths,
    draws, chol, spot, owner, tfactor, tset, notional, strike, out,
    chol_in, spot_in, owner_in, trades_in, trades_f_in, pack_a, pack_b,
    mine, over_y, y_sum, over_z, blocks, z_all, z_parts, prices, order, order_in, ends, ends_in,
    strikes, notionals, keeps, floors, nets, sums, over_x, x_sum, over_fy, fy_sum, over_fz,
    in_sems, order_sem, ends_sem, own_sem, y_send, y_recv, z_send, z_recv, x_send, x_recv,
    d_send, d_recv, fx_send, fx_recv, fy_send, fy_recv, fz_send, fz_recv,
):
    dates = 2 * sections
    section = lax.axis_index("section")
    place = lax.axis_index("paths")
    y, z = lax.div(place, zs), lax.rem(place, zs)
    y_peers = [(section, lax.rem(y + i, ys) * zs + z) for i in range(1, ys)]
    z_peers = [(section, y * zs + lax.rem(z + i, zs)) for i in range(1, zs)]
    x_peers = [(lax.rem(section + i, sections), place) for i in range(1, sections)]

    barrier = pltpu.get_barrier_semaphore()
    for peer in y_peers + z_peers + x_peers:
        pl.semaphore_signal(barrier, inc=1, device_id=peer, device_id_type=MESH)

    loads = [
        pltpu.make_async_copy(chol, chol_in, in_sems.at[0]),
        pltpu.make_async_copy(owner, owner_in, in_sems.at[1]),
        pltpu.make_async_copy(spot, spot_in, in_sems.at[2]),
        pltpu.make_async_copy(tfactor, trades_in.at[0], in_sems.at[3]),
        pltpu.make_async_copy(tset, trades_in.at[1], in_sems.at[4]),
        pltpu.make_async_copy(notional, trades_f_in.at[0], in_sems.at[5]),
        pltpu.make_async_copy(strike, trades_f_in.at[1], in_sems.at[6]),
    ]
    for load in loads:
        load.start()
    own = pltpu.make_async_copy(
        draws.at[:, :, pl.ds(pl.multiple_of(section * LANES, LANES), LANES)],
        z_all.at[section, pl.ds(0, factors)],
        own_sem,
    )
    own.start()

    pack_a[...] = jnp.zeros_like(pack_a)
    pack_b[...] = jnp.zeros_like(pack_b)
    for e in range(sections):
        z_all[e, factors:64] = jnp.zeros((64 - factors, 2, LANES), F32)
    loads[0].wait()
    loads[1].wait()
    pack_a[0:factors, 0:factors] = jnp.where(owner_in[2 * section] == place, chol_in[0, :, 0, :], 0.0)
    pack_b[0:factors, 0:factors] = jnp.where(owner_in[2 * section + 1] == place, chol_in[1, :, 0, :], 0.0)
    mine[...] = packed(pack_a[...], pack_b[...])

    pl.semaphore_wait(barrier, len(y_peers) + len(z_peers) + len(x_peers))

    def part(c):
        return pl.ds(c * (32 // CHUNKS), 32 // CHUNKS)

    def sends(peers, source, target, send, recv, c):
        copies = [
            remote(source.at[part(c)], target(i).at[part(c)], send.at[i, c], recv.at[i, c], peer)
            for i, peer in enumerate(peers)
        ]
        for copy in copies:
            copy.start()
        return copies

    to_y = [sends(y_peers, mine, lambda i: over_y.at[i], y_send, y_recv, c) for c in range(CHUNKS)]
    to_d = [
        remote(
            draws.at[:, :, pl.ds(pl.multiple_of(peer[0] * LANES, LANES), LANES)],
            z_all.at[section, pl.ds(0, factors)],
            d_send.at[i], d_recv.at[i], peer,
        )
        for i, peer in enumerate(x_peers)
    ]
    for copy in to_d:
        copy.start()

    for load in loads[2:]:
        load.wait()
    keys = [
        trades_in[1, 8 * v:8 * v + 8, :] * 64 + trades_in[0, 8 * v:8 * v + 8, :] for v in range(4)
    ]
    carried = [[trades_f_in[a, 8 * v:8 * v + 8, :] for v in range(4)] for a in range(2)]
    keys, (notional_s, strike_s) = in_set_order(keys, carried)
    wide = jnp.concatenate([k & 63 for k in keys] * 4, axis=0)
    order[...] = jnp.transpose(wide)
    to_order = pltpu.make_async_copy(order, order_in, order_sem)
    to_order.start()

    to_z = []
    for c in range(CHUNKS):
        total = mine[part(c), :]
        for i, copy in enumerate(to_y[c]):
            copy.wait_recv()
            total = total + over_y[i, part(c), :]
        y_sum[part(c), :] = total
        to_z.append(sends(z_peers, y_sum, lambda i: over_z.at[i], z_send, z_recv, c))

    set_s = [k >> 6 for k in keys]
    sub, lane = iota((8, LANES), 0), iota((8, LANES), 1)
    down = pltpu.roll(set_s[3], 1, 0)
    before = [jnp.where(sub == 0, pltpu.roll(down, 1, 1), down), set_s[0], set_s[1], set_s[2]]
    keep_s = []
    for v in range(4):
        same = jnp.where(before[v] == set_s[v], 1.0, 0.0)
        if v == 0:
            same = jnp.where((sub == 0) & ((lane == 0) | (lane == LANES // 2)), 0.0, same)
        keep_s.append(same)
    for c in range(LANES):
        for v in range(4):
            at = pl.ds(c * 32 + 8 * v, 8)
            strikes[at, :] = jnp.broadcast_to(strike_s[v][:, c:c + 1], (8, LANES))
            notionals[at, :] = jnp.broadcast_to(notional_s[v][:, c:c + 1], (8, LANES))
            keeps[at, :] = jnp.broadcast_to(keep_s[v][:, c:c + 1], (8, LANES))

    upto = [jnp.zeros((8, LANES), I32) for _ in range(SETS // LANES)]
    for c in range(LANES):
        for v in range(4):
            sets = jnp.broadcast_to(set_s[v][:, c:c + 1], (8, LANES))
            upto = [u + jnp.where(sets <= lane + b * LANES, 1, 0) for b, u in enumerate(upto)]
    for step in (4, 2, 1):
        upto = [u + pltpu.roll(u, step, 0) for u in upto]
    through = jnp.zeros((8, LANES), I32)
    start = jnp.zeros((8, LANES), I32)
    for b, u in enumerate(upto):
        through = jnp.where(sub == b, u, through)
        first = pltpu.roll(upto[b - 1], 1, 1) if b else jnp.zeros((8, LANES), I32)
        start = jnp.where(sub == b, jnp.where(lane == 0, first, pltpu.roll(u, 1, 1)), start)
    ends[0] = jnp.where(through > start, through - 1, TRADES)
    ends[1] = jnp.where((start < HALF) & (through > HALF), HALF - 1, TRADES)
    to_ends = pltpu.make_async_copy(ends, ends_in, ends_sem)
    to_ends.start()

    spots = jnp.concatenate([spot_in[...], jnp.zeros((1, LANES - factors), F32)], axis=1)
    level = jnp.transpose(jnp.broadcast_to(spots, (LANES, LANES)))[:64]
    nets[TRADES] = jnp.zeros((dates, LANES), F32)
    floors[TRADES] = jnp.zeros((1, LANES), F32)

    def some_floors(c, accs):
        accs = list(accs)
        for j in range(32):
            row = (j & 3) * 8 + (j >> 2)
            for half in range(2):
                column = c + half * (LANES // 2)
                at = pl.ds(column * 32 + row, 1)
                accs[half] = accs[half] * keeps[at, :] + notionals[at, :] * strikes[at, :]
                floors[column * 32 + j] = accs[half]
        return tuple(accs)

    none = jnp.zeros((1, LANES), F32)
    lax.fori_loop(0, LANES // 2, some_floors, (none, none))

    to_x = []
    for c in range(CHUNKS):
        total = y_sum[part(c), :]
        for i, copy in enumerate(to_z[c]):
            copy.wait_recv()
            total = total + over_z[i, part(c), :]
        blocks[section, part(c), :] = total
        to_x.append(
            sends(x_peers, blocks.at[section], lambda i: blocks.at[section], x_send, x_recv, c)
        )

    own.wait()
    for copy in to_d:
        copy.wait_recv()
    for e in range(sections):
        for d in range(2):
            high, rest = (part.astype(jnp.bfloat16) for part in halves(z_all[e, :, d, :]))
            z_parts[2 * e + d] = jnp.concatenate([high, high, rest, rest], axis=0)

    to_order.wait()
    to_ends.wait()
    for copies in to_x:
        for copy in copies:
            copy.wait_recv()

    for e in range(sections):
        for d, lower in enumerate(unpacked(blocks[e])):
            high, rest = halves(lower)
            both = (high + pltpu.roll(rest, 64, 1)).astype(jnp.bfloat16)
            level = level + jnp.dot(
                jnp.concatenate([both, both], axis=1), z_parts[2 * e + d], preferred_element_type=F32
            )
            prices[:, 2 * e + d, :] = jnp.exp(level)

    def some_trades(c, accs):
        accs = list(accs)
        for j in range(32):
            row = (j & 3) * 8 + (j >> 2)
            for half in range(2):
                column = c + half * (LANES // 2)
                at = pl.ds(column * 32 + row, 1)
                price = prices[order_in[column, row]]
                above = notionals[at, :] * jnp.maximum(price, strikes[at, :])
                accs[half] = accs[half] * keeps[at, :] + above
                nets[column * 32 + j] = accs[half]
        return tuple(accs)

    zero = jnp.zeros((dates, LANES), F32)
    lax.fori_loop(0, LANES // 2, some_trades, (zero, zero))

    lanes = iota((dates, LANES), 1)
    for b in range(SETS // LANES):
        sums_b = jnp.zeros((dates, LANES), F32)
        for at in range(LANES):
            last, halfway = ends_in[0, b, at], ends_in[1, b, at]
            floor = floors[last] + floors[halfway]
            net = nets[last] + nets[halfway] - floor
            sum_s = jnp.sum(jnp.maximum(net, 0.0), axis=1, keepdims=True)
            sums_b = jnp.where(lanes == at, sum_s, sums_b)
        for d in range(dates):
            sums[4 * d + b:4 * d + b + 1, :] = sums_b[d:d + 1]

    def rows_of(s):
        return sums.at[pl.ds(pl.multiple_of(s * 8, 8), 8), :]

    to_fx = [
        remote(rows_of(peer[0]), over_x.at[i], fx_send.at[i], fx_recv.at[i], peer)
        for i, peer in enumerate(x_peers)
    ]
    for copy in to_fx:
        copy.start()
    total = sums[pl.ds(pl.multiple_of(section * 8, 8), 8), :]
    for i, copy in enumerate(to_fx):
        copy.wait_recv()
        total = total + over_x[i]
    x_sum[...] = total
    to_fy = [
        remote(x_sum, over_fy.at[i], fy_send.at[i], fy_recv.at[i], peer)
        for i, peer in enumerate(y_peers)
    ]
    for copy in to_fy:
        copy.start()
    for i, copy in enumerate(to_fy):
        copy.wait_recv()
        total = total + over_fy[i]
    fy_sum[...] = total
    to_fz = [
        remote(fy_sum, over_fz.at[i], fz_send.at[i], fz_recv.at[i], peer)
        for i, peer in enumerate(z_peers)
    ]
    for copy in to_fz:
        copy.start()
    for i, copy in enumerate(to_fz):
        copy.wait_recv()
        total = total + over_fz[i]
    total = total / paths
    for d in range(2):
        for b in range(SETS // LANES):
            at = d * (SETS // LANES) + b
            out[d:d + 1, b * LANES:(b + 1) * LANES] = total[at:at + 1]
    for copies in (*to_y, *to_z, *to_x, to_d, to_fx, to_fy, to_fz):
        for copy in copies:
            copy.wait_send()


def shards(sections, ys, zs, normal_draws, cholesky, log_spot, owner, trade_factor, trade_set, notional, strike):
    factors = normal_draws.shape[1]
    dates = 2 * sections
    dma = pltpu.SemaphoreType.DMA
    vmem = pltpu.VMEM
    square = (ROWS, LANES)
    paths = normal_draws.shape[2] * ys * zs
    return pl.pallas_call(
        functools.partial(kernel, sections, ys, zs, factors, paths),
        out_shape=jax.ShapeDtypeStruct((2, SETS), F32),
        in_specs=[pl.BlockSpec(memory_space=pl.ANY)] * 8,
        out_specs=pl.BlockSpec(memory_space=pltpu.VMEM),
        scratch_shapes=[
            vmem((2, factors, 1, factors), F32),
            vmem((1, factors), F32),
            pltpu.SMEM((dates,), I32),
            vmem((2, *square), I32),
            vmem((2, *square), F32),
            vmem((LANES, LANES), F32),
            vmem((LANES, LANES), F32),
            vmem((32, LANES), F32),
            vmem((ys - 1, 32, LANES), F32),
            vmem((32, LANES), F32),
            vmem((zs - 1, 32, LANES), F32),
            vmem((sections, 32, LANES), F32),
            vmem((sections, 64, 2, LANES), F32),
            vmem((dates, 256, LANES), jnp.bfloat16),
            vmem((64, dates, LANES), F32),
            vmem((LANES, LANES), I32),
            pltpu.SMEM((LANES, LANES), I32),
            vmem((2, 8, LANES), I32),
            pltpu.SMEM((2, 8, LANES), I32),
            vmem((TRADES, LANES), F32),
            vmem((TRADES, LANES), F32),
            vmem((TRADES, LANES), F32),
            vmem((TRADES + 1, 1, LANES), F32),
            vmem((TRADES + 1, dates, LANES), F32),
            vmem((4 * dates, LANES), F32),
            vmem((sections - 1, 8, LANES), F32),
            vmem((8, LANES), F32),
            vmem((ys - 1, 8, LANES), F32),
            vmem((8, LANES), F32),
            vmem((zs - 1, 8, LANES), F32),
            dma((7,)), dma, dma, dma,
            dma((ys - 1, CHUNKS)), dma((ys - 1, CHUNKS)), dma((zs - 1, CHUNKS)), dma((zs - 1, CHUNKS)),
            dma((sections - 1, CHUNKS)), dma((sections - 1, CHUNKS)),
            dma((sections - 1,)), dma((sections - 1,)),
            dma((sections - 1,)), dma((sections - 1,)), dma((ys - 1,)), dma((ys - 1,)),
            dma((zs - 1,)), dma((zs - 1,)),
        ],
        compiler_params=pltpu.CompilerParams(
            collective_id=0, has_side_effects=True, vmem_limit_bytes=60 * 1024 * 1024
        ),
    )(
        jnp.transpose(normal_draws, (1, 0, 2)), jnp.transpose(cholesky, (0, 2, 1, 3)), log_spot.reshape(1, factors), owner,
        trade_factor.reshape(square), trade_set.reshape(square),
        notional.reshape(square), strike.reshape(square),
    )


def solution(mesh):
    placed = (
        P("section", None, "paths"),
        P("section", "paths", None, None),
        P(), P(), P(), P(), P(), P(),
    )
    sections, paths = mesh.shape["section"], mesh.shape["paths"]
    zs = 8 if paths == 32 else 2
    return jax.shard_map(
        functools.partial(shards, sections, paths // zs, zs),
        mesh=mesh, in_specs=placed, out_specs=P("section", None), check_vma=False,
    )
```

```python
import functools

import jax
import jax.numpy as jnp
from jax import lax
from jax.experimental import pallas as pl
from jax.experimental.pallas import tpu as pltpu
from jax.sharding import PartitionSpec as P

SETS = 512
TRADES = 4096
LANES = 128
ROWS = TRADES // LANES
HALF = TRADES // 2
CHUNKS = 1
MESH = pl.DeviceIdType.MESH
HIGHEST = lax.Precision.HIGHEST
F32 = jnp.float32
I32 = jnp.int32


def iota(shape, axis):
    return lax.broadcasted_iota(I32, shape, axis)


def farthest_first(n):
    return sorted(range(1, n), key=lambda i: -min(i, n - i))


def remote(src, dst, send, recv, device):
    return pltpu.make_async_remote_copy(
        src_ref=src, dst_ref=dst, send_sem=send, recv_sem=recv, device_id=device, device_id_type=MESH
    )


def packed(first, second):
    row, col = iota((64, LANES), 0), iota((64, LANES), 1)
    across = jnp.transpose(second)[:64]
    square = jnp.where(col <= row, first[:64], across)
    diagonal = jnp.sum(jnp.where(col == row, second[:64], 0.0), axis=0, keepdims=True)
    square = jnp.where(row == 60, diagonal, square)
    return jnp.where(col[:32] < 64, square[:32], pltpu.roll(square[32:], 64, 1))


def unpacked(both):
    row, col = iota((64, LANES), 0), iota((64, LANES), 1)
    square = jnp.concatenate([both, pltpu.roll(both, 64, 1)], axis=0)
    square = jnp.where(col < 64, square, 0.0)
    first = jnp.where((col <= row) & (row < 60), square, 0.0)
    across = jnp.transpose(jnp.concatenate([square, jnp.zeros_like(square)], axis=0))[:64]
    second = jnp.where(col < row, across, 0.0)
    second = jnp.where(col == row, square[60:61], second)
    return first, jnp.where(row < 60, second, 0.0)


def halves(x):
    high = x.astype(jnp.bfloat16).astype(F32)
    return high, x - high


def partner(x, bit):
    if bit < 2:
        step = 1 << bit
        return [x[place ^ step] for place in range(4)]
    axis, step, extent = (0, 1 << (bit - 2), 8) if bit < 5 else (1, 1 << (bit - 5), LANES)
    upper = (iota((8, LANES), axis) & step) != 0
    return [
        jnp.where(upper, pltpu.roll(v, step, axis), pltpu.roll(v, extent - step, axis)) for v in x
    ]


def place_bit(bit, vreg):
    if bit < 2:
        return jnp.full((8, LANES), (vreg >> bit) & 1, I32)
    axis, shift = (0, bit - 2) if bit < 5 else (1, bit - 5)
    return (iota((8, LANES), axis) >> shift) & 1


def in_set_order(keys, carried):
    for level in range(1, 13):
        for bit in range(level - 1, -1, -1):
            other = partner(keys, bit)
            others = [partner(c, bit) for c in carried]
            new_keys, news = [], [[] for _ in carried]
            for v in range(4):
                upward = place_bit(level, v) if level < 12 else jnp.zeros((8, LANES), I32)
                wants_small = place_bit(bit, v) == upward
                swap = jnp.where(wants_small, keys[v] - other[v], other[v] - keys[v]) > 0
                new_keys.append(jnp.where(swap, other[v], keys[v]))
                for new, c, o in zip(news, carried, others):
                    new.append(jnp.where(swap, o[v], c[v]))
            keys, carried = new_keys, news
    return keys, carried


def kernel(
    sections, ys, zs, factors, paths,
    draws, chol, spot, owner, tfactor, tset, notional, strike, out,
    chol_in, spot_in, owner_in, trades_in, trades_f_in, pack_a, pack_b,
    mine, over_y, y_sum, over_z, blocks, z_all, z_parts, prices, order, order_in, ends, ends_in,
    strikes, notionals, keeps, nets, sums, over_x, x_sum, over_fy, fy_sum, over_fz,
    in_sems, order_sem, ends_sem, own_sem, y_send, y_recv, z_send, z_recv, x_send, x_recv,
    d_send, d_recv, fx_send, fx_recv, fy_send, fy_recv, fz_send, fz_recv,
):
    dates = 2 * sections
    section = lax.axis_index("section")
    place = lax.axis_index("paths")
    y, z = lax.div(place, zs), lax.rem(place, zs)
    y_peers = [(section, lax.rem(y + i, ys) * zs + z) for i in farthest_first(ys)]
    z_peers = [(section, y * zs + lax.rem(z + i, zs)) for i in farthest_first(zs)]
    x_peers = [(lax.rem(section + i, sections), place) for i in farthest_first(sections)]

    barrier = pltpu.get_barrier_semaphore()
    for peer in z_peers + x_peers + y_peers:
        pl.semaphore_signal(barrier, inc=1, device_id=peer, device_id_type=MESH)

    loads = [
        pltpu.make_async_copy(chol, chol_in, in_sems.at[0]),
        pltpu.make_async_copy(owner, owner_in, in_sems.at[1]),
        pltpu.make_async_copy(spot, spot_in, in_sems.at[2]),
        pltpu.make_async_copy(tfactor, trades_in.at[0], in_sems.at[3]),
        pltpu.make_async_copy(tset, trades_in.at[1], in_sems.at[4]),
        pltpu.make_async_copy(notional, trades_f_in.at[0], in_sems.at[5]),
        pltpu.make_async_copy(strike, trades_f_in.at[1], in_sems.at[6]),
    ]
    for load in loads:
        load.start()
    own = pltpu.make_async_copy(
        draws.at[:, :, pl.ds(pl.multiple_of(section * LANES, LANES), LANES)],
        z_all.at[section, pl.ds(0, factors)],
        own_sem,
    )
    own.start()

    pack_a[...] = jnp.zeros_like(pack_a)
    pack_b[...] = jnp.zeros_like(pack_b)
    for e in range(sections):
        z_all[e, factors:64] = jnp.zeros((64 - factors, 2, LANES), F32)
    loads[0].wait()
    loads[1].wait()
    pack_a[0:factors, 0:factors] = jnp.where(owner_in[2 * section] == place, chol_in[0, :, 0, :], 0.0)
    pack_b[0:factors, 0:factors] = jnp.where(owner_in[2 * section + 1] == place, chol_in[1, :, 0, :], 0.0)
    mine[...] = packed(pack_a[...], pack_b[...])

    pl.semaphore_wait(barrier, len(y_peers) + len(z_peers) + len(x_peers))

    def part(c):
        return pl.ds(c * (32 // CHUNKS), 32 // CHUNKS)

    def sends(peers, source, target, send, recv, c):
        copies = [
            remote(source.at[part(c)], target(i).at[part(c)], send.at[i, c], recv.at[i, c], peer)
            for i, peer in enumerate(peers)
        ]
        for copy in copies:
            copy.start()
        return copies

    to_y = [sends(y_peers, mine, lambda i: over_y.at[i], y_send, y_recv, c) for c in range(CHUNKS)]
    to_d = [
        remote(
            draws.at[:, :, pl.ds(pl.multiple_of(peer[0] * LANES, LANES), LANES)],
            z_all.at[section, pl.ds(0, factors)],
            d_send.at[i], d_recv.at[i], peer,
        )
        for i, peer in enumerate(x_peers)
    ]
    for copy in to_d:
        copy.start()

    for load in loads[2:]:
        load.wait()
    keys = [
        trades_in[1, 8 * v:8 * v + 8, :] * 64 + trades_in[0, 8 * v:8 * v + 8, :] for v in range(4)
    ]
    carried = [[trades_f_in[a, 8 * v:8 * v + 8, :] for v in range(4)] for a in range(2)]
    keys, (notional_s, strike_s) = in_set_order(keys, carried)
    wide = jnp.concatenate([k & 63 for k in keys] * 4, axis=0)
    order[...] = jnp.transpose(wide)
    to_order = pltpu.make_async_copy(order, order_in, order_sem)
    to_order.start()

    to_z = []
    for c in range(CHUNKS):
        total = mine[part(c), :]
        for i, copy in enumerate(to_y[c]):
            copy.wait_recv()
            total = total + over_y[i, part(c), :]
        y_sum[part(c), :] = total
        to_z.append(sends(z_peers, y_sum, lambda i: over_z.at[i], z_send, z_recv, c))

    set_s = [k >> 6 for k in keys]
    sub, lane = iota((8, LANES), 0), iota((8, LANES), 1)
    down = pltpu.roll(set_s[3], 1, 0)
    before = [jnp.where(sub == 0, pltpu.roll(down, 1, 1), down), set_s[0], set_s[1], set_s[2]]
    keep_s = []
    for v in range(4):
        same = jnp.where(before[v] == set_s[v], 1.0, 0.0)
        if v == 0:
            same = jnp.where((sub == 0) & ((lane == 0) | (lane == LANES // 2)), 0.0, same)
        keep_s.append(same)
    for c in range(LANES):
        for v in range(4):
            at = pl.ds(c * 32 + 8 * v, 8)
            strikes[at, :] = jnp.broadcast_to(strike_s[v][:, c:c + 1], (8, LANES))
            notionals[at, :] = jnp.broadcast_to(notional_s[v][:, c:c + 1], (8, LANES))
            keeps[at, :] = jnp.broadcast_to(keep_s[v][:, c:c + 1], (8, LANES))

    upto = [jnp.zeros((8, LANES), I32) for _ in range(SETS // LANES)]
    for c in range(LANES):
        for v in range(4):
            sets = jnp.broadcast_to(set_s[v][:, c:c + 1], (8, LANES))
            upto = [u + jnp.where(sets <= lane + b * LANES, 1, 0) for b, u in enumerate(upto)]
    for step in (4, 2, 1):
        upto = [u + pltpu.roll(u, step, 0) for u in upto]
    through = jnp.zeros((8, LANES), I32)
    start = jnp.zeros((8, LANES), I32)
    for b, u in enumerate(upto):
        through = jnp.where(sub == b, u, through)
        first = pltpu.roll(upto[b - 1], 1, 1) if b else jnp.zeros((8, LANES), I32)
        start = jnp.where(sub == b, jnp.where(lane == 0, first, pltpu.roll(u, 1, 1)), start)
    ends[0] = jnp.where(through > start, through - 1, TRADES)
    ends[1] = jnp.where((start < HALF) & (through > HALF), HALF - 1, TRADES)
    to_ends = pltpu.make_async_copy(ends, ends_in, ends_sem)
    to_ends.start()

    spots = jnp.concatenate([spot_in[...], jnp.zeros((1, LANES - factors), F32)], axis=1)
    level = jnp.transpose(jnp.broadcast_to(spots, (LANES, LANES)))[:64]
    nets[TRADES] = jnp.zeros((dates, LANES), F32)

    to_x = []
    for c in range(CHUNKS):
        total = y_sum[part(c), :]
        for i, copy in enumerate(to_z[c]):
            copy.wait_recv()
            total = total + over_z[i, part(c), :]
        blocks[section, part(c), :] = total
        to_x.append(
            sends(x_peers, blocks.at[section], lambda i: blocks.at[section], x_send, x_recv, c)
        )

    own.wait()
    for copy in to_d:
        copy.wait_recv()
    for e in range(sections):
        for d in range(2):
            high, rest = (part.astype(jnp.bfloat16) for part in halves(z_all[e, :, d, :]))
            z_parts[2 * e + d] = jnp.concatenate([high, high, rest, rest], axis=0)

    to_order.wait()
    to_ends.wait()
    for copies in to_x:
        for copy in copies:
            copy.wait_recv()

    for e in range(sections):
        for d, lower in enumerate(unpacked(blocks[e])):
            high, rest = halves(lower)
            both = (high + pltpu.roll(rest, 64, 1)).astype(jnp.bfloat16)
            level = level + jnp.dot(
                jnp.concatenate([both, both], axis=1), z_parts[2 * e + d], preferred_element_type=F32
            )
            prices[:, 2 * e + d, :] = jnp.exp(level)

    def some_trades(c, accs):
        accs = list(accs)
        for j in range(32):
            row = (j & 3) * 8 + (j >> 2)
            for half in range(2):
                column = c + half * (LANES // 2)
                at = pl.ds(column * 32 + row, 1)
                price = prices[order_in[column, row]]
                payoff = notionals[at, :] * jnp.maximum(price - strikes[at, :], 0.0)
                accs[half] = accs[half] * keeps[at, :] + payoff
                nets[column * 32 + j] = accs[half]
        return tuple(accs)

    zero = jnp.zeros((dates, LANES), F32)
    lax.fori_loop(0, LANES // 2, some_trades, (zero, zero))

    lanes = iota((dates, LANES), 1)
    for b in range(SETS // LANES):
        sums_b = jnp.zeros((dates, LANES), F32)
        for at in range(LANES):
            last, halfway = ends_in[0, b, at], ends_in[1, b, at]
            net = nets[last] + nets[halfway]
            sum_s = jnp.sum(jnp.maximum(net, 0.0), axis=1, keepdims=True)
            sums_b = jnp.where(lanes == at, sum_s, sums_b)
        for d in range(dates):
            sums[4 * d + b:4 * d + b + 1, :] = sums_b[d:d + 1]

    def rows_of(s):
        return sums.at[pl.ds(pl.multiple_of(s * 8, 8), 8), :]

    to_fx = [
        remote(rows_of(peer[0]), over_x.at[i], fx_send.at[i], fx_recv.at[i], peer)
        for i, peer in enumerate(x_peers)
    ]
    for copy in to_fx:
        copy.start()
    total = sums[pl.ds(pl.multiple_of(section * 8, 8), 8), :]
    for i, copy in enumerate(to_fx):
        copy.wait_recv()
        total = total + over_x[i]
    x_sum[...] = total
    to_fy = [
        remote(x_sum, over_fy.at[i], fy_send.at[i], fy_recv.at[i], peer)
        for i, peer in enumerate(y_peers)
    ]
    for copy in to_fy:
        copy.start()
    for i, copy in enumerate(to_fy):
        copy.wait_recv()
        total = total + over_fy[i]
    fy_sum[...] = total
    to_fz = [
        remote(fy_sum, over_fz.at[i], fz_send.at[i], fz_recv.at[i], peer)
        for i, peer in enumerate(z_peers)
    ]
    for copy in to_fz:
        copy.start()
    for i, copy in enumerate(to_fz):
        copy.wait_recv()
        total = total + over_fz[i]
    total = total / paths
    for d in range(2):
        for b in range(SETS // LANES):
            at = d * (SETS // LANES) + b
            out[d:d + 1, b * LANES:(b + 1) * LANES] = total[at:at + 1]
    for copies in (*to_y, *to_z, *to_x, to_d, to_fx, to_fy, to_fz):
        for copy in copies:
            copy.wait_send()


def shards(sections, ys, zs, normal_draws, cholesky, log_spot, owner, trade_factor, trade_set, notional, strike):
    factors = normal_draws.shape[1]
    dates = 2 * sections
    dma = pltpu.SemaphoreType.DMA
    vmem = pltpu.VMEM
    square = (ROWS, LANES)
    paths = normal_draws.shape[2] * ys * zs
    return pl.pallas_call(
        functools.partial(kernel, sections, ys, zs, factors, paths),
        out_shape=jax.ShapeDtypeStruct((2, SETS), F32),
        in_specs=[pl.BlockSpec(memory_space=pl.ANY)] * 8,
        out_specs=pl.BlockSpec(memory_space=pltpu.VMEM),
        scratch_shapes=[
            vmem((2, factors, 1, factors), F32),
            vmem((1, factors), F32),
            pltpu.SMEM((dates,), I32),
            vmem((2, *square), I32),
            vmem((2, *square), F32),
            vmem((LANES, LANES), F32),
            vmem((LANES, LANES), F32),
            vmem((32, LANES), F32),
            vmem((ys - 1, 32, LANES), F32),
            vmem((32, LANES), F32),
            vmem((zs - 1, 32, LANES), F32),
            vmem((sections, 32, LANES), F32),
            vmem((sections, 64, 2, LANES), F32),
            vmem((dates, 256, LANES), jnp.bfloat16),
            vmem((64, dates, LANES), F32),
            vmem((LANES, LANES), I32),
            pltpu.SMEM((LANES, LANES), I32),
            vmem((2, 8, LANES), I32),
            pltpu.SMEM((2, 8, LANES), I32),
            vmem((TRADES, LANES), F32),
            vmem((TRADES, LANES), F32),
            vmem((TRADES, LANES), F32),
            vmem((TRADES + 1, dates, LANES), F32),
            vmem((4 * dates, LANES), F32),
            vmem((sections - 1, 8, LANES), F32),
            vmem((8, LANES), F32),
            vmem((ys - 1, 8, LANES), F32),
            vmem((8, LANES), F32),
            vmem((zs - 1, 8, LANES), F32),
            dma((7,)), dma, dma, dma,
            dma((ys - 1, CHUNKS)), dma((ys - 1, CHUNKS)), dma((zs - 1, CHUNKS)), dma((zs - 1, CHUNKS)),
            dma((sections - 1, CHUNKS)), dma((sections - 1, CHUNKS)),
            dma((sections - 1,)), dma((sections - 1,)),
            dma((sections - 1,)), dma((sections - 1,)), dma((ys - 1,)), dma((ys - 1,)),
            dma((zs - 1,)), dma((zs - 1,)),
        ],
        compiler_params=pltpu.CompilerParams(
            collective_id=0, has_side_effects=True, vmem_limit_bytes=60 * 1024 * 1024
        ),
    )(
        jnp.transpose(normal_draws, (1, 0, 2)), jnp.transpose(cholesky, (0, 2, 1, 3)), log_spot.reshape(1, factors), owner,
        trade_factor.reshape(square), trade_set.reshape(square),
        notional.reshape(square), strike.reshape(square),
    )


def solution(mesh):
    placed = (
        P("section", None, "paths"),
        P("section", "paths", None, None),
        P(), P(), P(), P(), P(), P(),
    )
    sections, paths = mesh.shape["section"], mesh.shape["paths"]
    zs = 8 if paths == 32 else 2
    return jax.shard_map(
        functools.partial(shards, sections, paths // zs, zs),
        mesh=mesh, in_specs=placed, out_specs=P("section", None), check_vma=False,
    )
```

```python
import functools

import jax
import jax.numpy as jnp
from jax import lax
from jax.experimental import pallas as pl
from jax.experimental.pallas import tpu as pltpu
from jax.sharding import PartitionSpec as P

SETS = 512
TRADES = 4096
LANES = 128
ROWS = TRADES // LANES
HALF = TRADES // 2
CHUNKS = 1
MESH = pl.DeviceIdType.MESH
HIGHEST = lax.Precision.HIGHEST
F32 = jnp.float32
I32 = jnp.int32


def iota(shape, axis):
    return lax.broadcasted_iota(I32, shape, axis)


def farthest_first(n):
    return sorted(range(1, n), key=lambda i: -min(i, n - i))


def remote(src, dst, send, recv, device):
    return pltpu.make_async_remote_copy(
        src_ref=src, dst_ref=dst, send_sem=send, recv_sem=recv, device_id=device, device_id_type=MESH
    )


def packed(first, second):
    row, col = iota((64, LANES), 0), iota((64, LANES), 1)
    across = jnp.transpose(second)[:64]
    square = jnp.where(col <= row, first[:64], across)
    diagonal = jnp.sum(jnp.where(col == row, second[:64], 0.0), axis=0, keepdims=True)
    square = jnp.where(row == 60, diagonal, square)
    return jnp.where(col[:32] < 64, square[:32], pltpu.roll(square[32:], 64, 1))


def unpacked(both):
    row, col = iota((64, LANES), 0), iota((64, LANES), 1)
    square = jnp.concatenate([both, pltpu.roll(both, 64, 1)], axis=0)
    square = jnp.where(col < 64, square, 0.0)
    first = jnp.where((col <= row) & (row < 60), square, 0.0)
    across = jnp.transpose(jnp.concatenate([square, jnp.zeros_like(square)], axis=0))[:64]
    second = jnp.where(col < row, across, 0.0)
    second = jnp.where(col == row, square[60:61], second)
    return first, jnp.where(row < 60, second, 0.0)


def halves(x):
    high = x.astype(jnp.bfloat16).astype(F32)
    return high, x - high


def partner(x, bit):
    if bit < 2:
        step = 1 << bit
        return [x[place ^ step] for place in range(4)]
    axis, step, extent = (0, 1 << (bit - 2), 8) if bit < 5 else (1, 1 << (bit - 5), LANES)
    upper = (iota((8, LANES), axis) & step) != 0
    return [
        jnp.where(upper, pltpu.roll(v, step, axis), pltpu.roll(v, extent - step, axis)) for v in x
    ]


def place_bit(bit, vreg):
    if bit < 2:
        return jnp.full((8, LANES), (vreg >> bit) & 1, I32)
    axis, shift = (0, bit - 2) if bit < 5 else (1, bit - 5)
    return (iota((8, LANES), axis) >> shift) & 1


def in_set_order(keys, carried):
    for level in range(1, 13):
        for bit in range(level - 1, -1, -1):
            other = partner(keys, bit)
            others = [partner(c, bit) for c in carried]
            new_keys, news = [], [[] for _ in carried]
            for v in range(4):
                upward = place_bit(level, v) if level < 12 else jnp.zeros((8, LANES), I32)
                wants_small = place_bit(bit, v) == upward
                swap = jnp.where(wants_small, keys[v] - other[v], other[v] - keys[v]) > 0
                new_keys.append(jnp.where(swap, other[v], keys[v]))
                for new, c, o in zip(news, carried, others):
                    new.append(jnp.where(swap, o[v], c[v]))
            keys, carried = new_keys, news
    return keys, carried


def kernel(
    sections, ys, zs, factors, paths,
    draws, chol, spot, owner, tfactor, tset, notional, strike, out,
    chol_in, spot_in, owner_in, trades_in, trades_f_in, pack_a, pack_b,
    mine, over_y, y_sum, over_z, blocks, z_all, z_parts, prices, order, order_in, ends, ends_in,
    strikes, notionals, keeps, nets, sums, over_x, x_sum, over_fy, fy_sum, over_fz,
    in_sems, order_sem, ends_sem, own_sem, y_send, y_recv, z_send, z_recv, x_send, x_recv,
    d_send, d_recv, fx_send, fx_recv, fy_send, fy_recv, fz_send, fz_recv,
):
    dates = 2 * sections
    section = lax.axis_index("section")
    place = lax.axis_index("paths")
    y, z = lax.div(place, zs), lax.rem(place, zs)
    y_peers = [(section, lax.rem(y + i, ys) * zs + z) for i in farthest_first(ys)]
    z_peers = [(section, y * zs + lax.rem(z + i, zs)) for i in farthest_first(zs)]
    x_peers = [(lax.rem(section + i, sections), place) for i in farthest_first(sections)]

    barrier = pltpu.get_barrier_semaphore()
    for peer in z_peers + x_peers + y_peers:
        pl.semaphore_signal(barrier, inc=1, device_id=peer, device_id_type=MESH)

    loads = [
        pltpu.make_async_copy(chol, chol_in, in_sems.at[0]),
        pltpu.make_async_copy(owner, owner_in, in_sems.at[1]),
        pltpu.make_async_copy(spot, spot_in, in_sems.at[2]),
        pltpu.make_async_copy(tfactor, trades_in.at[0], in_sems.at[3]),
        pltpu.make_async_copy(tset, trades_in.at[1], in_sems.at[4]),
        pltpu.make_async_copy(notional, trades_f_in.at[0], in_sems.at[5]),
        pltpu.make_async_copy(strike, trades_f_in.at[1], in_sems.at[6]),
    ]
    for load in loads:
        load.start()
    own = pltpu.make_async_copy(
        draws.at[:, :, pl.ds(pl.multiple_of(section * LANES, LANES), LANES)],
        z_all.at[section, pl.ds(0, factors)],
        own_sem,
    )
    own.start()

    pack_a[...] = jnp.zeros_like(pack_a)
    pack_b[...] = jnp.zeros_like(pack_b)
    for e in range(sections):
        z_all[e, factors:64] = jnp.zeros((64 - factors, 2, LANES), F32)
    loads[0].wait()
    loads[1].wait()
    pack_a[0:factors, 0:factors] = jnp.where(owner_in[2 * section] == place, chol_in[0, :, 0, :], 0.0)
    pack_b[0:factors, 0:factors] = jnp.where(owner_in[2 * section + 1] == place, chol_in[1, :, 0, :], 0.0)
    mine[...] = packed(pack_a[...], pack_b[...])

    pl.semaphore_wait(barrier, len(y_peers) + len(z_peers) + len(x_peers))

    def part(c):
        return pl.ds(c * (32 // CHUNKS), 32 // CHUNKS)

    def sends(peers, source, target, send, recv, c):
        copies = [
            remote(source.at[part(c)], target(i).at[part(c)], send.at[i, c], recv.at[i, c], peer)
            for i, peer in enumerate(peers)
        ]
        for copy in copies:
            copy.start()
        return copies

    to_y = [sends(y_peers, mine, lambda i: over_y.at[i], y_send, y_recv, c) for c in range(CHUNKS)]
    to_d = [
        remote(
            draws.at[:, :, pl.ds(pl.multiple_of(peer[0] * LANES, LANES), LANES)],
            z_all.at[section, pl.ds(0, factors)],
            d_send.at[i], d_recv.at[i], peer,
        )
        for i, peer in enumerate(x_peers)
    ]
    for copy in to_d:
        copy.start()

    to_z = []
    for c in range(CHUNKS):
        total = mine[part(c), :]
        for i, copy in enumerate(to_y[c]):
            copy.wait_recv()
            total = total + over_y[i, part(c), :]
        y_sum[part(c), :] = total
        to_z.append(sends(z_peers, y_sum, lambda i: over_z.at[i], z_send, z_recv, c))

    for load in loads[2:]:
        load.wait()
    keys = [
        trades_in[1, 8 * v:8 * v + 8, :] * 64 + trades_in[0, 8 * v:8 * v + 8, :] for v in range(4)
    ]
    carried = [[trades_f_in[a, 8 * v:8 * v + 8, :] for v in range(4)] for a in range(2)]
    keys, (notional_s, strike_s) = in_set_order(keys, carried)
    wide = jnp.concatenate([k & 63 for k in keys] * 4, axis=0)
    order[...] = jnp.transpose(wide)
    to_order = pltpu.make_async_copy(order, order_in, order_sem)
    to_order.start()

    set_s = [k >> 6 for k in keys]
    sub, lane = iota((8, LANES), 0), iota((8, LANES), 1)
    down = pltpu.roll(set_s[3], 1, 0)
    before = [jnp.where(sub == 0, pltpu.roll(down, 1, 1), down), set_s[0], set_s[1], set_s[2]]
    keep_s = []
    for v in range(4):
        same = jnp.where(before[v] == set_s[v], 1.0, 0.0)
        if v == 0:
            same = jnp.where((sub == 0) & ((lane == 0) | (lane == LANES // 2)), 0.0, same)
        keep_s.append(same)
    for c in range(LANES):
        for v in range(4):
            at = pl.ds(c * 32 + 8 * v, 8)
            strikes[at, :] = jnp.broadcast_to(strike_s[v][:, c:c + 1], (8, LANES))
            notionals[at, :] = jnp.broadcast_to(notional_s[v][:, c:c + 1], (8, LANES))
            keeps[at, :] = jnp.broadcast_to(keep_s[v][:, c:c + 1], (8, LANES))

    upto = [jnp.zeros((8, LANES), I32) for _ in range(SETS // LANES)]
    for c in range(LANES):
        for v in range(4):
            sets = jnp.broadcast_to(set_s[v][:, c:c + 1], (8, LANES))
            upto = [u + jnp.where(sets <= lane + b * LANES, 1, 0) for b, u in enumerate(upto)]
    for step in (4, 2, 1):
        upto = [u + pltpu.roll(u, step, 0) for u in upto]
    through = jnp.zeros((8, LANES), I32)
    start = jnp.zeros((8, LANES), I32)
    for b, u in enumerate(upto):
        through = jnp.where(sub == b, u, through)
        first = pltpu.roll(upto[b - 1], 1, 1) if b else jnp.zeros((8, LANES), I32)
        start = jnp.where(sub == b, jnp.where(lane == 0, first, pltpu.roll(u, 1, 1)), start)
    ends[0] = jnp.where(through > start, through - 1, TRADES)
    ends[1] = jnp.where((start < HALF) & (through > HALF), HALF - 1, TRADES)
    to_ends = pltpu.make_async_copy(ends, ends_in, ends_sem)
    to_ends.start()

    spots = jnp.concatenate([spot_in[...], jnp.zeros((1, LANES - factors), F32)], axis=1)
    level = jnp.transpose(jnp.broadcast_to(spots, (LANES, LANES)))[:64]
    nets[TRADES] = jnp.zeros((dates, LANES), F32)

    to_x = []
    for c in range(CHUNKS):
        total = y_sum[part(c), :]
        for i, copy in enumerate(to_z[c]):
            copy.wait_recv()
            total = total + over_z[i, part(c), :]
        blocks[section, part(c), :] = total
        to_x.append(
            sends(x_peers, blocks.at[section], lambda i: blocks.at[section], x_send, x_recv, c)
        )

    own.wait()
    for copy in to_d:
        copy.wait_recv()
    for e in range(sections):
        for d in range(2):
            high, rest = (part.astype(jnp.bfloat16) for part in halves(z_all[e, :, d, :]))
            z_parts[2 * e + d] = jnp.concatenate([high, high, rest, rest], axis=0)

    to_order.wait()
    to_ends.wait()
    for copies in to_x:
        for copy in copies:
            copy.wait_recv()

    for e in range(sections):
        for d, lower in enumerate(unpacked(blocks[e])):
            high, rest = halves(lower)
            both = (high + pltpu.roll(rest, 64, 1)).astype(jnp.bfloat16)
            level = level + jnp.dot(
                jnp.concatenate([both, both], axis=1), z_parts[2 * e + d], preferred_element_type=F32
            )
            prices[:, 2 * e + d, :] = jnp.exp(level)

    def some_trades(c, accs):
        accs = list(accs)
        for j in range(32):
            row = (j & 3) * 8 + (j >> 2)
            for half in range(2):
                column = c + half * (LANES // 2)
                at = pl.ds(column * 32 + row, 1)
                price = prices[order_in[column, row]]
                payoff = notionals[at, :] * jnp.maximum(price - strikes[at, :], 0.0)
                accs[half] = accs[half] * keeps[at, :] + payoff
                nets[column * 32 + j] = accs[half]
        return tuple(accs)

    zero = jnp.zeros((dates, LANES), F32)
    lax.fori_loop(0, LANES // 2, some_trades, (zero, zero), unroll=2)

    lanes = iota((dates, LANES), 1)
    for b in range(SETS // LANES):
        sums_b = jnp.zeros((dates, LANES), F32)
        for at in range(LANES):
            last, halfway = ends_in[0, b, at], ends_in[1, b, at]
            net = nets[last] + nets[halfway]
            sum_s = jnp.sum(jnp.maximum(net, 0.0), axis=1, keepdims=True)
            sums_b = jnp.where(lanes == at, sum_s, sums_b)
        for d in range(dates):
            sums[4 * d + b:4 * d + b + 1, :] = sums_b[d:d + 1]

    def rows_of(s):
        return sums.at[pl.ds(pl.multiple_of(s * 8, 8), 8), :]

    to_fx = [
        remote(rows_of(peer[0]), over_x.at[i], fx_send.at[i], fx_recv.at[i], peer)
        for i, peer in enumerate(x_peers)
    ]
    for copy in to_fx:
        copy.start()
    total = sums[pl.ds(pl.multiple_of(section * 8, 8), 8), :]
    for i, copy in enumerate(to_fx):
        copy.wait_recv()
        total = total + over_x[i]
    x_sum[...] = total
    to_fy = [
        remote(x_sum, over_fy.at[i], fy_send.at[i], fy_recv.at[i], peer)
        for i, peer in enumerate(y_peers)
    ]
    for copy in to_fy:
        copy.start()
    for i, copy in enumerate(to_fy):
        copy.wait_recv()
        total = total + over_fy[i]
    fy_sum[...] = total
    to_fz = [
        remote(fy_sum, over_fz.at[i], fz_send.at[i], fz_recv.at[i], peer)
        for i, peer in enumerate(z_peers)
    ]
    for copy in to_fz:
        copy.start()
    for i, copy in enumerate(to_fz):
        copy.wait_recv()
        total = total + over_fz[i]
    total = total / paths
    for d in range(2):
        for b in range(SETS // LANES):
            at = d * (SETS // LANES) + b
            out[d:d + 1, b * LANES:(b + 1) * LANES] = total[at:at + 1]
    for copies in (*to_y, *to_z, *to_x, to_d, to_fx, to_fy, to_fz):
        for copy in copies:
            copy.wait_send()


def shards(sections, ys, zs, normal_draws, cholesky, log_spot, owner, trade_factor, trade_set, notional, strike):
    factors = normal_draws.shape[1]
    dates = 2 * sections
    dma = pltpu.SemaphoreType.DMA
    vmem = pltpu.VMEM
    square = (ROWS, LANES)
    paths = normal_draws.shape[2] * ys * zs
    return pl.pallas_call(
        functools.partial(kernel, sections, ys, zs, factors, paths),
        out_shape=jax.ShapeDtypeStruct((2, SETS), F32),
        in_specs=[pl.BlockSpec(memory_space=pl.ANY)] * 8,
        out_specs=pl.BlockSpec(memory_space=pltpu.VMEM),
        scratch_shapes=[
            vmem((2, factors, 1, factors), F32),
            vmem((1, factors), F32),
            pltpu.SMEM((dates,), I32),
            vmem((2, *square), I32),
            vmem((2, *square), F32),
            vmem((LANES, LANES), F32),
            vmem((LANES, LANES), F32),
            vmem((32, LANES), F32),
            vmem((ys - 1, 32, LANES), F32),
            vmem((32, LANES), F32),
            vmem((zs - 1, 32, LANES), F32),
            vmem((sections, 32, LANES), F32),
            vmem((sections, 64, 2, LANES), F32),
            vmem((dates, 256, LANES), jnp.bfloat16),
            vmem((64, dates, LANES), F32),
            vmem((LANES, LANES), I32),
            pltpu.SMEM((LANES, LANES), I32),
            vmem((2, 8, LANES), I32),
            pltpu.SMEM((2, 8, LANES), I32),
            vmem((TRADES, LANES), F32),
            vmem((TRADES, LANES), F32),
            vmem((TRADES, LANES), F32),
            vmem((TRADES + 1, dates, LANES), F32),
            vmem((4 * dates, LANES), F32),
            vmem((sections - 1, 8, LANES), F32),
            vmem((8, LANES), F32),
            vmem((ys - 1, 8, LANES), F32),
            vmem((8, LANES), F32),
            vmem((zs - 1, 8, LANES), F32),
            dma((7,)), dma, dma, dma,
            dma((ys - 1, CHUNKS)), dma((ys - 1, CHUNKS)), dma((zs - 1, CHUNKS)), dma((zs - 1, CHUNKS)),
            dma((sections - 1, CHUNKS)), dma((sections - 1, CHUNKS)),
            dma((sections - 1,)), dma((sections - 1,)),
            dma((sections - 1,)), dma((sections - 1,)), dma((ys - 1,)), dma((ys - 1,)),
            dma((zs - 1,)), dma((zs - 1,)),
        ],
        compiler_params=pltpu.CompilerParams(
            collective_id=0, has_side_effects=True, vmem_limit_bytes=60 * 1024 * 1024
        ),
    )(
        jnp.transpose(normal_draws, (1, 0, 2)), jnp.transpose(cholesky, (0, 2, 1, 3)), log_spot.reshape(1, factors), owner,
        trade_factor.reshape(square), trade_set.reshape(square),
        notional.reshape(square), strike.reshape(square),
    )


def solution(mesh):
    placed = (
        P("section", None, "paths"),
        P("section", "paths", None, None),
        P(), P(), P(), P(), P(), P(),
    )
    sections, paths = mesh.shape["section"], mesh.shape["paths"]
    zs = 8 if paths == 32 else 2
    return jax.shard_map(
        functools.partial(shards, sections, paths // zs, zs),
        mesh=mesh, in_specs=placed, out_specs=P("section", None), check_vma=False,
    )
```
